32 devices in a mesh: pole: 2 (over y), prow: 4 (over z), pcol: 4 (over x, core).
Axes of the slice: x: 2, y: 2, z: 4, core: 2. Of those that a mesh axis runs over, the one named last changes fastest.
Arguments:
- ainv_anc: bfloat16 [2, 4096, 2048], P(None, ('pole', 'prow'), 'pcol'), parts along dimension 1, may hold values from -6 to 6
- panel: bfloat16 [2, 8, 1024, 256], P(None, 'pole', ('pcol', 'prow')), parts along dimension 1, may hold values from -6 to 6
- u_inv: bfloat16 [2, 8, 256, 256], P(None, 'pole'), parts along dimension 1, may hold values from -0.01171875 to 0.01171875
- k_inv: float32 [2, 8, 256, 256], P(None, ('pole', 'pcol')), parts along dimension 1, may hold values from -6 to 6
- structure: int32 [4, 4], replicated, may hold values from -1 to 7, as said below
Outputs:
- sel_inv: float32 [2, 4096, 1024], P(None, ('pole', 'prow'), 'pcol'), parts along dimension 1
- diag_inv: float32 [2, 8, 256, 256], P(None, ('pole', 'pcol')), parts along dimension 1
The draws below stay inside these ranges and needn't reach their ends.
There are 2 independent parts, one for each index of `pole`. The reference program is written for one: setup_inputs(seed, part) draws one part's arguments, and reference() takes and returns one part's arrays. A program takes and returns all parts, laid end to end along the dimension named above; an argument that names none is the same for every part. Nothing has to cross between parts.
Inputs may be any that keep to these rules, and one draw needn't show every extreme that they name: `structure`: slots g * 1 to (g + 1) * 1 - 1 of row k hold distinct blocks of g * 2 to (g + 1) * 2 - 1 in rising order, followed by -1 for empty slots; each such group of each row holds at least one block, and for every g some row fills all 1 slots of group g.
All inputs are finite; a program needn't handle non-finite values.
Results may differ from the reference program's by a relative error of at most 0.005.
Values may be sent and summed in bfloat16 or wider, within the bound.
A program may use at most 128 MiB of HBM per device.

```python
import jax
import jax.numpy as jnp
from jax import lax

B = 256
NS = 8
GROUPB = 2
M = 4
GSLOT = 1
NK = 4


def draw_structure(key, part):
    groups = NS // GROUPB
    key_count = jax.random.fold_in(key, 11)
    key_full = jax.random.fold_in(key, 12)
    key_score = jax.random.fold_in(key, 13)
    counts = jax.random.randint(key_count, (NK, groups), 1, GSLOT + 1)
    full_row = jax.random.randint(key_full, (groups,), 0, NK)
    counts = jnp.where(jnp.arange(NK)[:, None] == full_row[None, :], GSLOT, counts)
    scores = jax.random.randint(key_score, (NK, groups, GROUPB), 0, 1 << 20) * GROUPB + jnp.arange(GROUPB)[None, None, :]
    order = jnp.argsort(scores, axis=-1)
    chosen = order[:, :, :GSLOT]
    slot_index = jnp.arange(GSLOT)
    live_slot = slot_index[None, None, :] < counts[:, :, None]
    keyed = jnp.where(live_slot, chosen, GROUPB + slot_index[None, None, :])
    ranked = jnp.sort(keyed, axis=-1)
    offset = jnp.arange(groups)[None, :, None] * GROUPB
    result = jnp.where(ranked < GROUPB, ranked + offset, -1)
    return result.reshape(NK, groups * GSLOT).astype(jnp.int32)


def block_levels(key, shape, cuts, least, high):
    gain = 1.0
    for position, parts in cuts:
        steps = jax.random.uniform(jax.random.fold_in(jax.random.fold_in(key, 6), position), (parts,), jnp.float32, least / len(cuts), high / len(cuts))
        gain = gain * jnp.repeat(jnp.exp(steps), shape[position] // parts).reshape((-1,) + (1,) * (len(shape) - 1 - position))
    return gain


def noise(stream_key, shape, deviation, reach, pieces=(), kind=jnp.bfloat16):
    gain = block_levels(stream_key, shape, pieces, -0.22, 0.18) if pieces else 1.0
    values = jax.random.normal(stream_key, shape, jnp.float32) * deviation * gain
    return jnp.minimum(jnp.maximum(values, -reach), reach).astype(kind)


def setup_inputs(seed: int = 0, part: int = 0) -> dict:
    splits = jax.random.split(jax.random.key(seed), 6)
    part_splits = jax.random.split(jax.random.fold_in(splits[5], part), 6)
    return {
        "ainv_anc": noise(part_splits[0], (2, NS * B, NS * B), 1.0, 6.0, ((1, 4), (2, 4))),
        "panel": noise(part_splits[1], (2, NK, M * B, B), 1.0, 6.0, ((2, 16),)),
        "u_inv": noise(part_splits[2], (2, NK, B, B), (B * B * M) ** -0.5, 0.01171875),
        "k_inv": noise(part_splits[3], (2, NK, B, B), 1.0, 6.0, ((1, 4),), jnp.float32),
        "structure": draw_structure(jax.random.fold_in(splits[5], 71), part),
    }


def complex_dot(left, right):
    real = jnp.dot(left[0], right[0], preferred_element_type=jnp.float32) - jnp.dot(left[1], right[1], preferred_element_type=jnp.float32)
    imag = jnp.dot(left[0], right[1], preferred_element_type=jnp.float32) + jnp.dot(left[1], right[0], preferred_element_type=jnp.float32)
    return jnp.stack([real, imag])


def complex_tdot(left, right):
    highest = lax.Precision.HIGHEST
    real = jnp.dot(left[0].T, right[0], precision=highest) - jnp.dot(left[1].T, right[1], precision=highest)
    imag = jnp.dot(left[0].T, right[1], precision=highest) + jnp.dot(left[1].T, right[0], precision=highest)
    return jnp.stack([real, imag])


def reference(ainv_anc, panel, u_inv, k_inv, structure):
    highest = lax.Precision.HIGHEST
    blocks = ainv_anc.reshape(2, NS, B, NS, B)

    def one_node(items):
        panel_k, slot_ids, u_block, k_block = items
        live_slots = slot_ids >= 0
        safe_ids = jnp.where(live_slots, slot_ids, 0).astype(jnp.int32)
        live_rows = jnp.repeat(live_slots, B)
        scaled = complex_dot(panel_k, u_block)
        scaled = jnp.where(live_rows[None, :, None], scaled, 0.0).astype(jnp.bfloat16)
        picked = jnp.take(jnp.take(blocks, safe_ids, axis=1), safe_ids, axis=3).reshape(2, M * B, M * B)
        result = -complex_dot(picked, scaled)
        result = jnp.where(live_rows[None, :, None], result, 0.0)
        diag_k = k_block - complex_tdot(scaled.astype(jnp.float32), result)
        onehot = (slot_ids[:, None] == jnp.arange(NS, dtype=jnp.int32)[None, :]).astype(jnp.float32)
        dense = jnp.einsum("mj,cmab->cjab", onehot, result.reshape(2, M, B, B), precision=highest)
        return dense, diag_k

    items = (jnp.moveaxis(panel, 1, 0), structure, jnp.moveaxis(u_inv, 1, 0), jnp.moveaxis(k_inv, 1, 0))
    dense, diag_inv = lax.map(one_node, items)
    sel_inv = jnp.transpose(dense, (1, 2, 3, 0, 4)).reshape(2, NS * B, NK * B)
    return sel_inv, jnp.moveaxis(diag_inv, 0, 1)
```

```python
import functools

import jax
import jax.numpy as jnp
from jax import lax
from jax.experimental import pallas as pl
from jax.experimental.pallas import tpu as pltpu
from jax.sharding import PartitionSpec as P

BF16 = jnp.bfloat16
F32 = jnp.float32


def cdot(left, right, dims=(((1,), (0,)), ((), ()))):
    def single(x, y):
        return lax.dot_general(x, y, dims, preferred_element_type=F32)

    real = single(left[0], right[0]) - single(left[1], right[1])
    imag = single(left[0], right[1]) + single(left[1], right[0])
    return real, imag


def remote(src, dst, send_sem, recv_sem, where):
    return pltpu.make_async_remote_copy(
        src_ref=src,
        dst_ref=dst,
        send_sem=send_sem,
        recv_sem=recv_sem,
        device_id=where,
        device_id_type=pl.DeviceIdType.MESH,
    )


def kernel(
    n_rows, n_cols, table, a_hbm, panel_hbm, u_hbm, r_out, t_out,
    av, pv, uv, pr, gather, pick_out, pick_in, acc, qsend_buf, qrecv_buf, tot,
    local_sem, p_send, p_recv, a_send, a_recv, g_send, g_recv, q_send, q_recv, t_send, t_recv,
):
    row = lax.axis_index("prow")
    col = lax.axis_index("pcol")
    width = u_hbm.shape[-1]
    part = panel_hbm.shape[2]
    pairs = n_cols // 2
    row_blocks = a_hbm.shape[1] // width
    col_blocks = a_hbm.shape[2] // width

    def peer(unit):
        return ((col // 2 + unit // 2) % pairs) * 2 + (col + unit) % 2

    copy_p = pltpu.make_async_copy(panel_hbm, pv, local_sem.at[0])
    copy_u = pltpu.make_async_copy(u_hbm.at[:, col], uv, local_sem.at[1])
    copy_a = pltpu.make_async_copy(a_hbm, av, local_sem.at[2])
    copy_p.start()
    copy_u.start()
    copy_a.start()

    barrier = pltpu.get_barrier_semaphore()
    for unit in range(1, n_cols):
        pl.semaphore_signal(barrier, inc=1, device_id={"pcol": peer(unit)}, device_id_type=pl.DeviceIdType.MESH)
    for step in range(1, n_rows):
        pl.semaphore_signal(
            barrier, inc=1, device_id={"prow": (row + step) % n_rows}, device_id_type=pl.DeviceIdType.MESH
        )
    pl.semaphore_wait(barrier, n_cols + n_rows - 2)

    def panel_copy(unit, source):
        return remote(
            pv.at[:, peer(unit)], pr.at[source], p_send.at[unit], p_recv.at[source], {"pcol": peer(unit)}
        )

    def pick_copy(unit, source):
        return remote(
            pick_out.at[unit], pick_in.at[source], a_send.at[unit], a_recv.at[source], {"pcol": peer(unit)}
        )

    def line_copy(unit, chunk, step, side):
        block = gather.at[unit, :, chunk]
        there = row + 1 if side == 0 else row - 1
        return remote(block, block, g_send.at[unit, side, step], g_recv.at[unit, chunk], {"prow": there})

    copy_p.wait()
    for unit in range(1, n_cols):
        panel_copy(unit, col).start()
    copy_u.wait()

    def scale(unit):
        slot = peer(unit)
        if unit == 0:
            left = (pv[0, col], pv[1, col])
        else:
            panel_copy(unit, slot).wait_recv()
            left = (pr[slot, 0], pr[slot, 1])
        real, imag = cdot(left, (uv[0], uv[1]))
        live = (jnp.full((1, width), table[col, slot]) >= 0).astype(F32)
        gather[unit, 0, row] = (real * live).astype(BF16)
        gather[unit, 1, row] = (imag * live).astype(BF16)

        @pl.when(row < n_rows - 1)
        def _():
            line_copy(unit, row, 0, 0).start()

        @pl.when(row > 0)
        def _():
            line_copy(unit, row, 0, 1).start()

    def pick(unit):
        node = peer(unit)
        top = jnp.full((1, width), table[node, row]) - row * row_blocks
        side = jnp.full((1, width), table[node, col]) - col * col_blocks
        for plane in range(2):
            total = None
            for i in range(row_blocks):
                for j in range(col_blocks):
                    keep = ((top == i) & (side == j)).astype(F32).astype(BF16)
                    block = av[plane, i * width : (i + 1) * width, j * width : (j + 1) * width] * keep
                    total = block if total is None else total + block
            pick_out[unit, plane] = total

    scale(0)
    scale(1)
    copy_a.wait()
    order = list(range(2, n_cols)) + [1]
    for unit in order:
        pick(unit)
        pick_copy(unit, col).start()
    pick(0)
    for unit in range(2, n_cols):
        scale(unit)

    for unit in range(n_cols):
        for step in range(1, n_rows):
            below, above = row - step, row + step

            @pl.when(below >= 0)
            def _():
                line_copy(unit, below, step, 0).wait_recv()

                @pl.when(row < n_rows - 1)
                def _():
                    line_copy(unit, below, step, 0).start()

            @pl.when(above <= n_rows - 1)
            def _():
                line_copy(unit, above, step, 1).wait_recv()

                @pl.when(row > 0)
                def _():
                    line_copy(unit, above, step, 1).start()

        slot = peer(unit)
        if unit == 0:
            left = (pick_out[0, 0], pick_out[0, 1])
        else:
            pick_copy(unit, slot).wait_recv()
            left = (pick_in[slot, 0], pick_in[slot, 1])
        right = tuple(gather[unit, plane].reshape(width, width) for plane in range(2))
        real, imag = cdot(left, right)
        if unit == 0:
            acc[0] = real
            acc[1] = imag
        else:
            acc[0] += real
            acc[1] += imag

    live = (jnp.full((1, width), table[col, row]) >= 0).astype(F32)
    unit_here = ((row // 2 - col // 2 + pairs) % pairs) * 2 + (row + col) % 2
    z = tuple(gather[unit_here, plane].reshape(width, width) for plane in range(2))
    r = (acc[0] * live, acc[1] * live)
    r_out[0] = r[0]
    r_out[1] = r[1]
    real, imag = cdot(z, (r[0].astype(BF16), r[1].astype(BF16)), (((0,), (0,)), ((), ())))
    acc[0] = real
    acc[1] = imag
    for plane in range(2):
        qsend_buf[:, plane] = acc[plane].reshape(n_rows, part, width).astype(BF16)

    def quad_copy(step, source):
        there = (row + step) % n_rows
        return remote(qsend_buf.at[there], qrecv_buf.at[source], q_send.at[step], q_recv.at[source], {"prow": there})

    def total_copy(step, source):
        there = (row + step) % n_rows
        return remote(tot.at[source], tot.at[source], t_send.at[step], t_recv.at[source], {"prow": there})

    for step in range(1, n_rows):
        quad_copy(step, row).start()
    mine = pl.ds(pl.multiple_of(row * part, part), part)
    sums = [acc[0, mine, :], acc[1, mine, :]]
    for step in range(1, n_rows):
        source = (row + step) % n_rows
        quad_copy(step, source).wait_recv()
        for plane in range(2):
            sums[plane] = sums[plane] + qrecv_buf[source, plane].astype(F32)
    for plane in range(2):
        tot[row, plane] = sums[plane].astype(BF16)
    for step in range(1, n_rows):
        total_copy(step, row).start()
    for step in range(1, n_rows):
        total_copy(step, (row + step) % n_rows).wait_recv()
    for plane in range(2):
        t_out[plane] = tot[:, plane].reshape(width, width)

    for unit in range(1, n_cols):
        panel_copy(unit, col).wait_send()
        pick_copy(unit, col).wait_send()
    for unit in range(n_cols):
        for step in range(n_rows):
            below, above = row - step, row + step

            @pl.when((below >= 0) & (row < n_rows - 1))
            def _():
                line_copy(unit, below, step, 0).wait_send()

            @pl.when((above <= n_rows - 1) & (row > 0))
            def _():
                line_copy(unit, above, step, 1).wait_send()

    for step in range(1, n_rows):
        quad_copy(step, row).wait_send()
        total_copy(step, row).wait_send()


def compact(ainv_anc, panel, u_inv, k_inv, structure):
    n_rows, n_cols = lax.axis_size("prow"), lax.axis_size("pcol")
    width, part = u_inv.shape[-1], panel.shape[2]
    row_blocks = ainv_anc.shape[1] // width
    hbm = pl.BlockSpec(memory_space=pl.ANY)
    vmem = pl.BlockSpec(memory_space=pltpu.VMEM)
    dma = pltpu.SemaphoreType.DMA
    r, total = pl.pallas_call(
        functools.partial(kernel, n_rows, n_cols),
        out_shape=(
            jax.ShapeDtypeStruct((2, width, width), F32),
            jax.ShapeDtypeStruct((2, width, width), BF16),
        ),
        in_specs=[pl.BlockSpec(memory_space=pltpu.SMEM), hbm, hbm, hbm],
        out_specs=(vmem, vmem),
        scratch_shapes=[
            pltpu.VMEM(ainv_anc.shape, BF16),
            pltpu.VMEM(panel.shape, BF16),
            pltpu.VMEM((2, width, width), BF16),
            pltpu.VMEM((n_cols, 2, part, width), BF16),
            pltpu.VMEM((n_cols, 2, n_rows, part, width), BF16),
            pltpu.VMEM((n_cols, 2, width, width), BF16),
            pltpu.VMEM((n_cols, 2, width, width), BF16),
            pltpu.VMEM((2, width, width), F32),
            pltpu.VMEM((n_rows, 2, part, width), BF16),
            pltpu.VMEM((n_rows, 2, part, width), BF16),
            pltpu.VMEM((n_rows, 2, part, width), BF16),
            dma((3,)),
            dma((n_cols,)),
            dma((n_cols,)),
            dma((n_cols,)),
            dma((n_cols,)),
            dma((n_cols, 2, n_rows)),
            dma((n_cols, n_rows)),
            dma((n_rows,)),
            dma((n_rows,)),
            dma((n_rows,)),
            dma((n_rows,)),
        ],
        compiler_params=pltpu.CompilerParams(
            collective_id=0, has_side_effects=True, vmem_limit_bytes=24 * 1024 * 1024
        ),
    )(structure, ainv_anc, panel, u_inv)
    row, col = lax.axis_index("prow"), lax.axis_index("pcol")
    named = structure[col, row] - row * row_blocks
    keep = named == jnp.arange(row_blocks, dtype=jnp.int32)
    sel_inv = jnp.where(keep[None, :, None, None], -r[:, None], 0.0)
    diag_inv = k_inv + total[:, None].astype(F32)
    return sel_inv.reshape(2, row_blocks * width, width), diag_inv


def complex_quad(z_part, s_part):
    highest = lax.Precision.HIGHEST

    def single(left, right):
        return jnp.einsum("kra,rkb->kab", left, right, precision=highest)

    real = single(z_part[0], s_part[0]) - single(z_part[1], s_part[1])
    imag = single(z_part[0], s_part[1]) + single(z_part[1], s_part[0])
    return jnp.stack([real, imag])


def local(ainv_anc, panel, u_inv, k_inv, structure):
    block_width = u_inv.shape[-1]
    cols = lax.axis_size("pcol")
    if (
        structure.shape[1] == cols
        and lax.axis_size("prow") == cols
        and ainv_anc.shape[1] == ainv_anc.shape[2]
        and u_inv.shape[1] == cols
        and cols % 2 == 0
    ):
        return compact(ainv_anc, panel, u_inv, k_inv, structure)
    total_k = u_inv.shape[1]
    own_k = k_inv.shape[1]
    n_cols = lax.axis_size("pcol")
    row_here = lax.axis_index("prow")
    col_here = lax.axis_index("pcol")
    row_blocks = ainv_anc.shape[1] // block_width
    group_blocks = ainv_anc.shape[2] // block_width
    group_slots = structure.shape[1] // n_cols
    rows_all = row_blocks * block_width
    col_struct = lax.dynamic_slice_in_dim(structure, col_here * group_slots, group_slots, 1)
    slot_live = col_struct >= 0
    slot_pos = col_struct - col_here * group_blocks
    first_block = row_here * row_blocks
    target = first_block + jnp.arange(row_blocks, dtype=jnp.int32)
    rows_in = lax.all_gather(panel, "prow", axis=2, tiled=True)

    def single(left, right):
        return jnp.einsum("knb,kbc->knc", left, right, preferred_element_type=jnp.float32)

    real = single(rows_in[0], u_inv[0]) - single(rows_in[1], u_inv[1])
    imag = single(rows_in[0], u_inv[1]) + single(rows_in[1], u_inv[0])
    placed = jnp.stack([real, imag]).astype(jnp.bfloat16)
    placed = placed.reshape(2, total_k, group_slots, block_width, block_width)
    placed = jnp.where(slot_live[None, :, :, None, None], placed, jnp.zeros((), jnp.bfloat16))
    block_ids = jnp.arange(group_blocks, dtype=jnp.int32)
    pick_table = (slot_pos[:, :, None] == block_ids[None, None, :]).astype(jnp.bfloat16)
    ainv_blocks = ainv_anc.reshape(2, rows_all, group_blocks, block_width)

    def one_node(items):
        table_k, rows_k = items
        picked = jnp.einsum(
            "sg,cigw->cisw", table_k, ainv_blocks, preferred_element_type=jnp.float32
        )
        picked = picked.astype(jnp.bfloat16).reshape(2, rows_all, group_slots * block_width)
        right = rows_k.reshape(2, group_slots * block_width, block_width)
        real = jnp.dot(picked[0], right[0], preferred_element_type=jnp.float32) - jnp.dot(
            picked[1], right[1], preferred_element_type=jnp.float32
        )
        imag = jnp.dot(picked[0], right[1], preferred_element_type=jnp.float32) + jnp.dot(
            picked[1], right[0], preferred_element_type=jnp.float32
        )
        return jnp.stack([real, imag])

    per_node = lax.map(one_node, (pick_table, jnp.moveaxis(placed, 1, 0)))
    partial_value = jnp.transpose(per_node, (1, 2, 0, 3))
    row_table = (col_struct[:, None, :] == target[None, :, None]).astype(jnp.bfloat16)
    z_rows = jnp.einsum("kts,ckswb->cktwb", row_table, placed, preferred_element_type=jnp.float32)
    z_rows = z_rows.astype(jnp.bfloat16).reshape(2, total_k, rows_all, block_width)
    summed = lax.psum_scatter(
        partial_value.reshape(2, rows_all, total_k * block_width),
        "pcol",
        scatter_dimension=2,
        tiled=True,
    )
    own_struct = lax.dynamic_slice_in_dim(structure, col_here * own_k, own_k, 0)
    member = jnp.any(own_struct[:, :, None] == target[None, None, :], axis=1)
    selected = -summed.reshape(2, row_blocks, block_width, own_k, block_width)
    selected = jnp.where(member.T[None, :, None, :, None], selected, 0.0)
    sel_inv = selected.reshape(2, rows_all, own_k * block_width)
    received = lax.all_to_all(z_rows, "pcol", split_axis=1, concat_axis=1, tiled=True)
    z_own = (
        received.astype(jnp.float32).reshape(2, n_cols, own_k, rows_all, block_width).sum(axis=1)
    )
    quad_term = complex_quad(z_own, selected.reshape(2, rows_all, own_k, block_width))
    total_sum = lax.psum(quad_term, "prow")
    diag_inv = k_inv - total_sum
    return (sel_inv, diag_inv)


def solution(mesh):
    placed = (
        P(None, ("pole", "prow"), "pcol"),
        P(None, "pole", ("pcol", "prow"), None),
        P(None, "pole", None, None),
        P(None, ("pole", "pcol"), None, None),
        P(),
    )
    return jax.shard_map(
        local,
        mesh=mesh,
        in_specs=placed,
        out_specs=(P(None, ("pole", "prow"), "pcol"), P(None, ("pole", "pcol"), None, None)),
        check_vma=False,
    )
```

```python
import functools

import jax
import jax.numpy as jnp
from jax import lax
from jax.experimental import pallas as pl
from jax.experimental.pallas import tpu as pltpu
from jax.sharding import PartitionSpec as P

BF16 = jnp.bfloat16
F32 = jnp.float32


def cdot(left, right, dims=(((1,), (0,)), ((), ()))):
    def single(x, y):
        return lax.dot_general(x, y, dims, preferred_element_type=F32)

    real = single(left[0], right[0]) - single(left[1], right[1])
    imag = single(left[0], right[1]) + single(left[1], right[0])
    return real, imag


def remote(src, dst, send_sem, recv_sem, where):
    return pltpu.make_async_remote_copy(
        src_ref=src,
        dst_ref=dst,
        send_sem=send_sem,
        recv_sem=recv_sem,
        device_id=where,
        device_id_type=pl.DeviceIdType.MESH,
    )


def kernel(
    n_rows, n_cols, table, a_hbm, panel_hbm, u_hbm, k_hbm, sel_out, diag_out,
    av, pv, uv, pr, gather, pick_out, pick_in, acc, r_buf, sel_buf, kv, qsend_buf, qrecv_buf, tot,
    local_sem, p_send, p_recv, a_send, a_recv, g_send, g_recv, q_send, q_recv, t_send, t_recv,
):
    row = lax.axis_index("prow")
    col = lax.axis_index("pcol")
    width = u_hbm.shape[-1]
    part = panel_hbm.shape[2]
    pairs = n_cols // 2
    row_blocks = a_hbm.shape[1] // width
    col_blocks = a_hbm.shape[2] // width

    def peer(unit):
        return ((col // 2 + unit // 2) % pairs) * 2 + (col + unit) % 2

    copy_p = pltpu.make_async_copy(panel_hbm, pv, local_sem.at[0])
    copy_u = pltpu.make_async_copy(u_hbm.at[:, col], uv, local_sem.at[1])
    copy_a = pltpu.make_async_copy(a_hbm, av, local_sem.at[2])
    copy_k = pltpu.make_async_copy(k_hbm, kv, local_sem.at[3])
    copy_p.start()
    copy_u.start()
    copy_a.start()
    copy_k.start()

    barrier = pltpu.get_barrier_semaphore()
    for unit in range(1, n_cols):
        pl.semaphore_signal(barrier, inc=1, device_id={"pcol": peer(unit)}, device_id_type=pl.DeviceIdType.MESH)
    for step in range(1, n_rows):
        pl.semaphore_signal(
            barrier, inc=1, device_id={"prow": (row + step) % n_rows}, device_id_type=pl.DeviceIdType.MESH
        )
    pl.semaphore_wait(barrier, n_cols + n_rows - 2)

    def panel_copy(unit, source):
        return remote(
            pv.at[:, peer(unit)], pr.at[source], p_send.at[unit], p_recv.at[source], {"pcol": peer(unit)}
        )

    def pick_copy(unit, source):
        return remote(
            pick_out.at[unit], pick_in.at[source], a_send.at[unit], a_recv.at[source], {"pcol": peer(unit)}
        )

    def line_copy(unit, chunk, step, side):
        block = gather.at[unit, :, chunk]
        there = row + 1 if side == 0 else row - 1
        return remote(block, block, g_send.at[unit, side, step], g_recv.at[unit, chunk], {"prow": there})

    copy_p.wait()
    for unit in range(1, n_cols):
        panel_copy(unit, col).start()
    copy_u.wait()

    def scale(unit):
        slot = peer(unit)
        if unit == 0:
            left = (pv[0, col], pv[1, col])
        else:
            panel_copy(unit, slot).wait_recv()
            left = (pr[slot, 0], pr[slot, 1])
        real, imag = cdot(left, (uv[0], uv[1]))
        live = (jnp.full((1, width), table[col, slot]) >= 0).astype(F32)
        gather[unit, 0, row] = (real * live).astype(BF16)
        gather[unit, 1, row] = (imag * live).astype(BF16)

        @pl.when(row < n_rows - 1)
        def _():
            line_copy(unit, row, 0, 0).start()

        @pl.when(row > 0)
        def _():
            line_copy(unit, row, 0, 1).start()

    def pick(unit):
        node = peer(unit)
        top = jnp.full((1, width), table[node, row]) - row * row_blocks
        side = jnp.full((1, width), table[node, col]) - col * col_blocks
        for plane in range(2):
            total = None
            for i in range(row_blocks):
                for j in range(col_blocks):
                    keep = ((top == i) & (side == j)).astype(F32).astype(BF16)
                    block = av[plane, i * width : (i + 1) * width, j * width : (j + 1) * width] * keep
                    total = block if total is None else total + block
            pick_out[unit, plane] = total

    scale(0)
    scale(1)
    copy_a.wait()
    order = list(range(2, n_cols)) + [1]
    for unit in order:
        pick(unit)
        pick_copy(unit, col).start()
    pick(0)

    def forward(unit, step):
        below, above = row - step, row + step

        @pl.when(below >= 0)
        def _():
            line_copy(unit, below, step, 0).wait_recv()

            @pl.when(row < n_rows - 1)
            def _():
                line_copy(unit, below, step, 0).start()

        @pl.when(above <= n_rows - 1)
        def _():
            line_copy(unit, above, step, 1).wait_recv()

            @pl.when(row > 0)
            def _():
                line_copy(unit, above, step, 1).start()

    def multiply(unit):
        slot = peer(unit)
        if unit == 0:
            left = (pick_out[0, 0], pick_out[0, 1])
        else:
            pick_copy(unit, slot).wait_recv()
            left = (pick_in[slot, 0], pick_in[slot, 1])
        right = tuple(gather[unit, plane].reshape(width, width) for plane in range(2))
        real, imag = cdot(left, right)
        if unit == 0:
            acc[0] = real
            acc[1] = imag
        else:
            acc[0] += real
            acc[1] += imag

    early, late = (0, 1), range(2, n_cols)
    for unit in early:
        forward(unit, 1)
    for unit in late:
        scale(unit)
    for step in range(2, n_rows + 1):
        for unit in early:
            if step < n_rows:
                forward(unit, step)
        for unit in late:
            forward(unit, step - 1)
        if step == n_rows - 1:
            for unit in early:
                multiply(unit)
    for unit in late:
        multiply(unit)

    live = (jnp.full((1, width), table[col, row]) >= 0).astype(F32)
    unit_here = ((row // 2 - col // 2 + pairs) % pairs) * 2 + (row + col) % 2
    z = tuple(gather[unit_here, plane].reshape(width, width) for plane in range(2))
    r = (acc[0] * live, acc[1] * live)
    r_buf[0] = r[0]
    r_buf[1] = r[1]
    real, imag = cdot(z, (r[0].astype(BF16), r[1].astype(BF16)), (((0,), (0,)), ((), ())))
    acc[0] = real
    acc[1] = imag
    for plane in range(2):
        qsend_buf[:, plane] = acc[plane].reshape(n_rows, part, width).astype(BF16)

    def quad_copy(step, source):
        there = (row + step) % n_rows
        return remote(qsend_buf.at[there], qrecv_buf.at[source], q_send.at[step], q_recv.at[source], {"prow": there})

    def total_copy(step, source):
        there = (row + step) % n_rows
        return remote(tot.at[source], tot.at[source], t_send.at[step], t_recv.at[source], {"prow": there})

    for step in range(1, n_rows):
        quad_copy(step, row).start()
    named = jnp.full((1, width), table[col, row]) - row * row_blocks
    for i in range(row_blocks):
        keep = -(named == i).astype(F32)
        for plane in range(2):
            sel_buf[plane, i * width : (i + 1) * width, :] = r_buf[plane] * keep
    copy_s = pltpu.make_async_copy(sel_buf, sel_out, local_sem.at[4])
    copy_s.start()
    copy_k.wait()
    mine = pl.ds(pl.multiple_of(row * part, part), part)
    sums = [acc[0, mine, :], acc[1, mine, :]]
    for step in range(1, n_rows):
        source = (row + step) % n_rows
        quad_copy(step, source).wait_recv()
        for plane in range(2):
            sums[plane] = sums[plane] + qrecv_buf[source, plane].astype(F32)
    for plane in range(2):
        tot[row, plane] = sums[plane].astype(BF16)
    for step in range(1, n_rows):
        total_copy(step, row).start()
    for step in range(1, n_rows):
        total_copy(step, (row + step) % n_rows).wait_recv()
    for plane in range(2):
        diag_out[plane, 0] = kv[plane, 0] + tot[:, plane].reshape(width, width).astype(F32)

    copy_s.wait()
    for unit in range(1, n_cols):
        panel_copy(unit, col).wait_send()
        pick_copy(unit, col).wait_send()
    for unit in range(n_cols):
        for step in range(n_rows):
            below, above = row - step, row + step

            @pl.when((below >= 0) & (row < n_rows - 1))
            def _():
                line_copy(unit, below, step, 0).wait_send()

            @pl.when((above <= n_rows - 1) & (row > 0))
            def _():
                line_copy(unit, above, step, 1).wait_send()

    for step in range(1, n_rows):
        quad_copy(step, row).wait_send()
        total_copy(step, row).wait_send()


def compact(ainv_anc, panel, u_inv, k_inv, structure):
    n_rows, n_cols = lax.axis_size("prow"), lax.axis_size("pcol")
    width, part = u_inv.shape[-1], panel.shape[2]
    row_blocks = ainv_anc.shape[1] // width
    hbm = pl.BlockSpec(memory_space=pltpu.HBM)
    vmem = pl.BlockSpec(memory_space=pltpu.VMEM)
    dma = pltpu.SemaphoreType.DMA
    return pl.pallas_call(
        functools.partial(kernel, n_rows, n_cols),
        out_shape=(
            jax.ShapeDtypeStruct((2, row_blocks * width, width), F32),
            jax.ShapeDtypeStruct(k_inv.shape, F32),
        ),
        in_specs=[pl.BlockSpec(memory_space=pltpu.SMEM), hbm, hbm, hbm, hbm],
        out_specs=(hbm, vmem),
        scratch_shapes=[
            pltpu.VMEM(ainv_anc.shape, BF16),
            pltpu.VMEM(panel.shape, BF16),
            pltpu.VMEM((2, width, width), BF16),
            pltpu.VMEM((n_cols, 2, part, width), BF16),
            pltpu.VMEM((n_cols, 2, n_rows, part, width), BF16),
            pltpu.VMEM((n_cols, 2, width, width), BF16),
            pltpu.VMEM((n_cols, 2, width, width), BF16),
            pltpu.VMEM((2, width, width), F32),
            pltpu.VMEM((2, width, width), F32),
            pltpu.VMEM((2, row_blocks * width, width), F32),
            pltpu.VMEM(k_inv.shape, F32),
            pltpu.VMEM((n_rows, 2, part, width), BF16),
            pltpu.VMEM((n_rows, 2, part, width), BF16),
            pltpu.VMEM((n_rows, 2, part, width), BF16),
            dma((5,)),
            dma((n_cols,)),
            dma((n_cols,)),
            dma((n_cols,)),
            dma((n_cols,)),
            dma((n_cols, 2, n_rows)),
            dma((n_cols, n_rows)),
            dma((n_rows,)),
            dma((n_rows,)),
            dma((n_rows,)),
            dma((n_rows,)),
        ],
        compiler_params=pltpu.CompilerParams(
            collective_id=0, has_side_effects=True
        ),
    )(structure, ainv_anc, panel, u_inv, k_inv)


def complex_quad(z_part, s_part):
    highest = lax.Precision.HIGHEST

    def single(left, right):
        return jnp.einsum("kra,rkb->kab", left, right, precision=highest)

    real = single(z_part[0], s_part[0]) - single(z_part[1], s_part[1])
    imag = single(z_part[0], s_part[1]) + single(z_part[1], s_part[0])
    return jnp.stack([real, imag])


def local(ainv_anc, panel, u_inv, k_inv, structure):
    block_width = u_inv.shape[-1]
    cols = lax.axis_size("pcol")
    if (
        structure.shape[1] == cols
        and lax.axis_size("prow") == cols
        and ainv_anc.shape[1] == ainv_anc.shape[2]
        and u_inv.shape[1] == cols
        and cols % 2 == 0
    ):
        return compact(ainv_anc, panel, u_inv, k_inv, structure)
    total_k = u_inv.shape[1]
    own_k = k_inv.shape[1]
    n_cols = lax.axis_size("pcol")
    row_here = lax.axis_index("prow")
    col_here = lax.axis_index("pcol")
    row_blocks = ainv_anc.shape[1] // block_width
    group_blocks = ainv_anc.shape[2] // block_width
    group_slots = structure.shape[1] // n_cols
    rows_all = row_blocks * block_width
    col_struct = lax.dynamic_slice_in_dim(structure, col_here * group_slots, group_slots, 1)
    slot_live = col_struct >= 0
    slot_pos = col_struct - col_here * group_blocks
    first_block = row_here * row_blocks
    target = first_block + jnp.arange(row_blocks, dtype=jnp.int32)
    rows_in = lax.all_gather(panel, "prow", axis=2, tiled=True)

    def single(left, right):
        return jnp.einsum("knb,kbc->knc", left, right, preferred_element_type=jnp.float32)

    real = single(rows_in[0], u_inv[0]) - single(rows_in[1], u_inv[1])
    imag = single(rows_in[0], u_inv[1]) + single(rows_in[1], u_inv[0])
    placed = jnp.stack([real, imag]).astype(jnp.bfloat16)
    placed = placed.reshape(2, total_k, group_slots, block_width, block_width)
    placed = jnp.where(slot_live[None, :, :, None, None], placed, jnp.zeros((), jnp.bfloat16))
    block_ids = jnp.arange(group_blocks, dtype=jnp.int32)
    pick_table = (slot_pos[:, :, None] == block_ids[None, None, :]).astype(jnp.bfloat16)
    ainv_blocks = ainv_anc.reshape(2, rows_all, group_blocks, block_width)

    def one_node(items):
        table_k, rows_k = items
        picked = jnp.einsum(
            "sg,cigw->cisw", table_k, ainv_blocks, preferred_element_type=jnp.float32
        )
        picked = picked.astype(jnp.bfloat16).reshape(2, rows_all, group_slots * block_width)
        right = rows_k.reshape(2, group_slots * block_width, block_width)
        real = jnp.dot(picked[0], right[0], preferred_element_type=jnp.float32) - jnp.dot(
            picked[1], right[1], preferred_element_type=jnp.float32
        )
        imag = jnp.dot(picked[0], right[1], preferred_element_type=jnp.float32) + jnp.dot(
            picked[1], right[0], preferred_element_type=jnp.float32
        )
        return jnp.stack([real, imag])

    per_node = lax.map(one_node, (pick_table, jnp.moveaxis(placed, 1, 0)))
    partial_value = jnp.transpose(per_node, (1, 2, 0, 3))
    row_table = (col_struct[:, None, :] == target[None, :, None]).astype(jnp.bfloat16)
    z_rows = jnp.einsum("kts,ckswb->cktwb", row_table, placed, preferred_element_type=jnp.float32)
    z_rows = z_rows.astype(jnp.bfloat16).reshape(2, total_k, rows_all, block_width)
    summed = lax.psum_scatter(
        partial_value.reshape(2, rows_all, total_k * block_width),
        "pcol",
        scatter_dimension=2,
        tiled=True,
    )
    own_struct = lax.dynamic_slice_in_dim(structure, col_here * own_k, own_k, 0)
    member = jnp.any(own_struct[:, :, None] == target[None, None, :], axis=1)
    selected = -summed.reshape(2, row_blocks, block_width, own_k, block_width)
    selected = jnp.where(member.T[None, :, None, :, None], selected, 0.0)
    sel_inv = selected.reshape(2, rows_all, own_k * block_width)
    received = lax.all_to_all(z_rows, "pcol", split_axis=1, concat_axis=1, tiled=True)
    z_own = (
        received.astype(jnp.float32).reshape(2, n_cols, own_k, rows_all, block_width).sum(axis=1)
    )
    quad_term = complex_quad(z_own, selected.reshape(2, rows_all, own_k, block_width))
    total_sum = lax.psum(quad_term, "prow")
    diag_inv = k_inv - total_sum
    return (sel_inv, diag_inv)


def solution(mesh):
    placed = (
        P(None, ("pole", "prow"), "pcol"),
        P(None, "pole", ("pcol", "prow"), None),
        P(None, "pole", None, None),
        P(None, ("pole", "pcol"), None, None),
        P(),
    )
    return jax.shard_map(
        local,
        mesh=mesh,
        in_specs=placed,
        out_specs=(P(None, ("pole", "prow"), "pcol"), P(None, ("pole", "pcol"), None, None)),
        check_vma=False,
    )
```

```python
import functools

import jax
import jax.numpy as jnp
from jax import lax
from jax.experimental import pallas as pl
from jax.experimental.pallas import tpu as pltpu
from jax.sharding import PartitionSpec as P

BF16 = jnp.bfloat16
F32 = jnp.float32


def cdot(left, right, dims=(((1,), (0,)), ((), ()))):
    def single(x, y):
        return lax.dot_general(x, y, dims, preferred_element_type=F32)

    real = single(left[0], right[0]) - single(left[1], right[1])
    imag = single(left[0], right[1]) + single(left[1], right[0])
    return real, imag


def remote(src, dst, send_sem, recv_sem, where):
    return pltpu.make_async_remote_copy(
        src_ref=src,
        dst_ref=dst,
        send_sem=send_sem,
        recv_sem=recv_sem,
        device_id=where,
        device_id_type=pl.DeviceIdType.MESH,
    )


def kernel(
    n_rows, n_cols, table, a_hbm, panel_hbm, u_hbm, k_hbm, sel_out, diag_out,
    av, pv, uv, pr, gather, pick_out, pick_in, acc, r_buf, sel_buf, kv, qsend_buf, qrecv_buf, tot,
    local_sem, p_send, p_recv, a_send, a_recv, g_send, g_recv, q_send, q_recv, t_send, t_recv,
):
    row = lax.axis_index("prow")
    col = lax.axis_index("pcol")
    width = u_hbm.shape[-1]
    part = panel_hbm.shape[2]
    pairs = n_cols // 2
    row_blocks = a_hbm.shape[1] // width
    col_blocks = a_hbm.shape[2] // width

    def peer(unit):
        return ((col // 2 + unit // 2) % pairs) * 2 + (col + unit) % 2

    copy_p = pltpu.make_async_copy(panel_hbm, pv, local_sem.at[0])
    copy_u = pltpu.make_async_copy(u_hbm.at[:, col], uv, local_sem.at[1])
    copy_a = pltpu.make_async_copy(a_hbm, av, local_sem.at[2])
    copy_k = pltpu.make_async_copy(k_hbm, kv, local_sem.at[3])
    copy_p.start()
    copy_u.start()
    copy_a.start()
    copy_k.start()

    barrier = pltpu.get_barrier_semaphore()
    for unit in range(1, n_cols):
        pl.semaphore_signal(barrier, inc=1, device_id={"pcol": peer(unit)}, device_id_type=pl.DeviceIdType.MESH)

    @pl.when(row > 0)
    def _():
        pl.semaphore_signal(barrier, inc=1, device_id={"prow": row - 1}, device_id_type=pl.DeviceIdType.MESH)

    @pl.when(row < n_rows - 1)
    def _():
        pl.semaphore_signal(barrier, inc=1, device_id={"prow": row + 1}, device_id_type=pl.DeviceIdType.MESH)

    ends = (row == 0).astype(jnp.int32) + (row == n_rows - 1).astype(jnp.int32)
    pl.semaphore_wait(barrier, n_cols + 1 - ends)

    def panel_copy(unit, source):
        return remote(
            pv.at[:, peer(unit)], pr.at[source], p_send.at[unit], p_recv.at[source], {"pcol": peer(unit)}
        )

    def pick_copy(unit, source):
        return remote(
            pick_out.at[unit], pick_in.at[source], a_send.at[unit], a_recv.at[source], {"pcol": peer(unit)}
        )

    def line_copy(unit, chunk, step, side):
        block = gather.at[unit, :, chunk]
        there = row + 1 if side == 0 else row - 1
        return remote(block, block, g_send.at[unit, side, step], g_recv.at[unit, chunk], {"prow": there})

    copy_p.wait()
    for unit in range(1, n_cols):
        panel_copy(unit, col).start()
    copy_u.wait()

    def scale(unit):
        slot = peer(unit)
        if unit == 0:
            left = (pv[0, col], pv[1, col])
        else:
            panel_copy(unit, slot).wait_recv()
            left = (pr[slot, 0], pr[slot, 1])
        real, imag = cdot(left, (uv[0], uv[1]))
        live = (jnp.full((1, width), table[col, slot]) >= 0).astype(F32)
        gather[unit, 0, row] = (real * live).astype(BF16)
        gather[unit, 1, row] = (imag * live).astype(BF16)

        @pl.when(row < n_rows - 1)
        def _():
            line_copy(unit, row, 0, 0).start()

        @pl.when(row > 0)
        def _():
            line_copy(unit, row, 0, 1).start()

    def pick(unit):
        node = peer(unit)
        top = jnp.full((1, width), table[node, row]) - row * row_blocks
        side = jnp.full((1, width), table[node, col]) - col * col_blocks
        for plane in range(2):
            total = None
            for i in range(row_blocks):
                for j in range(col_blocks):
                    keep = ((top == i) & (side == j)).astype(F32).astype(BF16)
                    block = av[plane, i * width : (i + 1) * width, j * width : (j + 1) * width] * keep
                    total = block if total is None else total + block
            pick_out[unit, plane] = total

    scale(0)
    scale(1)
    copy_a.wait()
    order = list(range(2, n_cols)) + [1]
    for unit in order:
        pick(unit)
        pick_copy(unit, col).start()
    pick(0)

    def forward(unit, step):
        below, above = row - step, row + step

        @pl.when(below >= 0)
        def _():
            line_copy(unit, below, step, 0).wait_recv()

            @pl.when(row < n_rows - 1)
            def _():
                line_copy(unit, below, step, 0).start()

        @pl.when(above <= n_rows - 1)
        def _():
            line_copy(unit, above, step, 1).wait_recv()

            @pl.when(row > 0)
            def _():
                line_copy(unit, above, step, 1).start()

    def multiply(unit):
        slot = peer(unit)
        if unit == 0:
            left = (pick_out[0, 0], pick_out[0, 1])
        else:
            pick_copy(unit, slot).wait_recv()
            left = (pick_in[slot, 0], pick_in[slot, 1])
        right = tuple(gather[unit, plane].reshape(width, width) for plane in range(2))
        real, imag = cdot(left, right)
        if unit == 0:
            acc[0] = real
            acc[1] = imag
        else:
            acc[0] += real
            acc[1] += imag

    early, late = (0, 1), range(2, n_cols)
    for unit in early:
        forward(unit, 1)
    for unit in late:
        scale(unit)
    for step in range(2, n_rows + 1):
        for unit in early:
            if step < n_rows:
                forward(unit, step)
        for unit in late:
            forward(unit, step - 1)
            if step == n_rows:
                multiply(unit)
        if step == n_rows - 1:
            for unit in early:
                multiply(unit)
    live = (jnp.full((1, width), table[col, row]) >= 0).astype(F32)
    unit_here = ((row // 2 - col // 2 + pairs) % pairs) * 2 + (row + col) % 2
    z = tuple(gather[unit_here, plane].reshape(width, width) for plane in range(2))
    r = (acc[0] * live, acc[1] * live)
    r_buf[0] = r[0]
    r_buf[1] = r[1]
    halves = 2
    half_width = width // halves

    def quad_copy(half, step, source):
        there = (row + step) % n_rows
        return remote(
            qsend_buf.at[half, there], qrecv_buf.at[half, source],
            q_send.at[half, step], q_recv.at[half, source], {"prow": there},
        )

    def total_copy(half, step, source):
        there = (row + step) % n_rows
        block = tot.at[half, source]
        return remote(block, block, t_send.at[half, step], t_recv.at[half, source], {"prow": there})

    low = (r[0].astype(BF16), r[1].astype(BF16))
    for half in range(halves):
        columns = slice(half * half_width, (half + 1) * half_width)
        quad = cdot(z, (low[0][:, columns], low[1][:, columns]), (((0,), (0,)), ((), ())))
        for plane in range(2):
            acc[plane, :, columns] = quad[plane]
            qsend_buf[half, :, plane] = quad[plane].reshape(n_rows, part, half_width).astype(BF16)
        for step in range(1, n_rows):
            quad_copy(half, step, row).start()
    named = jnp.full((1, width), table[col, row]) - row * row_blocks
    for i in range(row_blocks):
        keep = -(named == i).astype(F32)
        for plane in range(2):
            sel_buf[plane, i * width : (i + 1) * width, :] = r_buf[plane] * keep
    copy_s = pltpu.make_async_copy(sel_buf, sel_out, local_sem.at[4])
    copy_s.start()
    copy_k.wait()
    mine = pl.ds(pl.multiple_of(row * part, part), part)
    for half in range(halves):
        columns = slice(half * half_width, (half + 1) * half_width)
        sums = [acc[0, mine, columns], acc[1, mine, columns]]
        for step in range(1, n_rows):
            source = (row + step) % n_rows
            quad_copy(half, step, source).wait_recv()
            for plane in range(2):
                sums[plane] = sums[plane] + qrecv_buf[half, source, plane].astype(F32)
        for plane in range(2):
            tot[half, row, plane] = sums[plane].astype(BF16)
        for step in range(1, n_rows):
            total_copy(half, step, row).start()
    for half in range(halves):
        columns = slice(half * half_width, (half + 1) * half_width)
        for step in range(1, n_rows):
            total_copy(half, step, (row + step) % n_rows).wait_recv()
        for plane in range(2):
            diag_out[plane, 0, :, columns] = (
                kv[plane, 0, :, columns] + tot[half, :, plane].reshape(width, half_width).astype(F32)
            )

    copy_s.wait()
    for unit in range(1, n_cols):
        panel_copy(unit, col).wait_send()
        pick_copy(unit, col).wait_send()
    for unit in range(n_cols):
        for step in range(n_rows):
            below, above = row - step, row + step

            @pl.when((below >= 0) & (row < n_rows - 1))
            def _():
                line_copy(unit, below, step, 0).wait_send()

            @pl.when((above <= n_rows - 1) & (row > 0))
            def _():
                line_copy(unit, above, step, 1).wait_send()

    for step in range(1, n_rows):
        for half in range(halves):
            quad_copy(half, step, row).wait_send()
            total_copy(half, step, row).wait_send()


def compact(ainv_anc, panel, u_inv, k_inv, structure):
    n_rows, n_cols = lax.axis_size("prow"), lax.axis_size("pcol")
    width, part = u_inv.shape[-1], panel.shape[2]
    row_blocks = ainv_anc.shape[1] // width
    hbm = pl.BlockSpec(memory_space=pltpu.HBM)
    vmem = pl.BlockSpec(memory_space=pltpu.VMEM)
    dma = pltpu.SemaphoreType.DMA
    return pl.pallas_call(
        functools.partial(kernel, n_rows, n_cols),
        out_shape=(
            jax.ShapeDtypeStruct((2, row_blocks * width, width), F32),
            jax.ShapeDtypeStruct(k_inv.shape, F32),
        ),
        in_specs=[pl.BlockSpec(memory_space=pltpu.SMEM), hbm, hbm, hbm, hbm],
        out_specs=(hbm, vmem),
        scratch_shapes=[
            pltpu.VMEM(ainv_anc.shape, BF16),
            pltpu.VMEM(panel.shape, BF16),
            pltpu.VMEM((2, width, width), BF16),
            pltpu.VMEM((n_cols, 2, part, width), BF16),
            pltpu.VMEM((n_cols, 2, n_rows, part, width), BF16),
            pltpu.VMEM((n_cols, 2, width, width), BF16),
            pltpu.VMEM((n_cols, 2, width, width), BF16),
            pltpu.VMEM((2, width, width), F32),
            pltpu.VMEM((2, width, width), F32),
            pltpu.VMEM((2, row_blocks * width, width), F32),
            pltpu.VMEM(k_inv.shape, F32),
            pltpu.VMEM((2, n_rows, 2, part, width // 2), BF16),
            pltpu.VMEM((2, n_rows, 2, part, width // 2), BF16),
            pltpu.VMEM((2, n_rows, 2, part, width // 2), BF16),
            dma((5,)),
            dma((n_cols,)),
            dma((n_cols,)),
            dma((n_cols,)),
            dma((n_cols,)),
            dma((n_cols, 2, n_rows)),
            dma((n_cols, n_rows)),
            dma((2, n_rows)),
            dma((2, n_rows)),
            dma((2, n_rows)),
            dma((2, n_rows)),
        ],
        compiler_params=pltpu.CompilerParams(
            collective_id=0, has_side_effects=True
        ),
    )(structure, ainv_anc, panel, u_inv, k_inv)


def complex_quad(z_part, s_part):
    highest = lax.Precision.HIGHEST

    def single(left, right):
        return jnp.einsum("kra,rkb->kab", left, right, precision=highest)

    real = single(z_part[0], s_part[0]) - single(z_part[1], s_part[1])
    imag = single(z_part[0], s_part[1]) + single(z_part[1], s_part[0])
    return jnp.stack([real, imag])


def local(ainv_anc, panel, u_inv, k_inv, structure):
    block_width = u_inv.shape[-1]
    cols = lax.axis_size("pcol")
    if (
        structure.shape[1] == cols
        and lax.axis_size("prow") == cols
        and ainv_anc.shape[1] == ainv_anc.shape[2]
        and u_inv.shape[1] == cols
        and cols % 2 == 0
    ):
        return compact(ainv_anc, panel, u_inv, k_inv, structure)
    total_k = u_inv.shape[1]
    own_k = k_inv.shape[1]
    n_cols = lax.axis_size("pcol")
    row_here = lax.axis_index("prow")
    col_here = lax.axis_index("pcol")
    row_blocks = ainv_anc.shape[1] // block_width
    group_blocks = ainv_anc.shape[2] // block_width
    group_slots = structure.shape[1] // n_cols
    rows_all = row_blocks * block_width
    col_struct = lax.dynamic_slice_in_dim(structure, col_here * group_slots, group_slots, 1)
    slot_live = col_struct >= 0
    slot_pos = col_struct - col_here * group_blocks
    first_block = row_here * row_blocks
    target = first_block + jnp.arange(row_blocks, dtype=jnp.int32)
    rows_in = lax.all_gather(panel, "prow", axis=2, tiled=True)

    def single(left, right):
        return jnp.einsum("knb,kbc->knc", left, right, preferred_element_type=jnp.float32)

    real = single(rows_in[0], u_inv[0]) - single(rows_in[1], u_inv[1])
    imag = single(rows_in[0], u_inv[1]) + single(rows_in[1], u_inv[0])
    placed = jnp.stack([real, imag]).astype(jnp.bfloat16)
    placed = placed.reshape(2, total_k, group_slots, block_width, block_width)
    placed = jnp.where(slot_live[None, :, :, None, None], placed, jnp.zeros((), jnp.bfloat16))
    block_ids = jnp.arange(group_blocks, dtype=jnp.int32)
    pick_table = (slot_pos[:, :, None] == block_ids[None, None, :]).astype(jnp.bfloat16)
    ainv_blocks = ainv_anc.reshape(2, rows_all, group_blocks, block_width)

    def one_node(items):
        table_k, rows_k = items
        picked = jnp.einsum(
            "sg,cigw->cisw", table_k, ainv_blocks, preferred_element_type=jnp.float32
        )
        picked = picked.astype(jnp.bfloat16).reshape(2, rows_all, group_slots * block_width)
        right = rows_k.reshape(2, group_slots * block_width, block_width)
        real = jnp.dot(picked[0], right[0], preferred_element_type=jnp.float32) - jnp.dot(
            picked[1], right[1], preferred_element_type=jnp.float32
        )
        imag = jnp.dot(picked[0], right[1], preferred_element_type=jnp.float32) + jnp.dot(
            picked[1], right[0], preferred_element_type=jnp.float32
        )
        return jnp.stack([real, imag])

    per_node = lax.map(one_node, (pick_table, jnp.moveaxis(placed, 1, 0)))
    partial_value = jnp.transpose(per_node, (1, 2, 0, 3))
    row_table = (col_struct[:, None, :] == target[None, :, None]).astype(jnp.bfloat16)
    z_rows = jnp.einsum("kts,ckswb->cktwb", row_table, placed, preferred_element_type=jnp.float32)
    z_rows = z_rows.astype(jnp.bfloat16).reshape(2, total_k, rows_all, block_width)
    summed = lax.psum_scatter(
        partial_value.reshape(2, rows_all, total_k * block_width),
        "pcol",
        scatter_dimension=2,
        tiled=True,
    )
    own_struct = lax.dynamic_slice_in_dim(structure, col_here * own_k, own_k, 0)
    member = jnp.any(own_struct[:, :, None] == target[None, None, :], axis=1)
    selected = -summed.reshape(2, row_blocks, block_width, own_k, block_width)
    selected = jnp.where(member.T[None, :, None, :, None], selected, 0.0)
    sel_inv = selected.reshape(2, rows_all, own_k * block_width)
    received = lax.all_to_all(z_rows, "pcol", split_axis=1, concat_axis=1, tiled=True)
    z_own = (
        received.astype(jnp.float32).reshape(2, n_cols, own_k, rows_all, block_width).sum(axis=1)
    )
    quad_term = complex_quad(z_own, selected.reshape(2, rows_all, own_k, block_width))
    total_sum = lax.psum(quad_term, "prow")
    diag_inv = k_inv - total_sum
    return (sel_inv, diag_inv)


def solution(mesh):
    placed = (
        P(None, ("pole", "prow"), "pcol"),
        P(None, "pole", ("pcol", "prow"), None),
        P(None, "pole", None, None),
        P(None, ("pole", "pcol"), None, None),
        P(),
    )
    return jax.shard_map(
        local,
        mesh=mesh,
        in_specs=placed,
        out_specs=(P(None, ("pole", "prow"), "pcol"), P(None, ("pole", "pcol"), None, None)),
        check_vma=False,
    )
```

```python
import functools

import jax
import jax.numpy as jnp
from jax import lax
from jax.experimental import pallas as pl
from jax.experimental.pallas import tpu as pltpu
from jax.sharding import PartitionSpec as P

BF16 = jnp.bfloat16
F32 = jnp.float32


def cdot(left, right, dims=(((1,), (0,)), ((), ()))):
    def single(x, y):
        return lax.dot_general(x, y, dims, preferred_element_type=F32)

    real = single(left[0], right[0]) - single(left[1], right[1])
    imag = single(left[0], right[1]) + single(left[1], right[0])
    return real, imag


def remote(src, dst, send_sem, recv_sem, where):
    return pltpu.make_async_remote_copy(
        src_ref=src,
        dst_ref=dst,
        send_sem=send_sem,
        recv_sem=recv_sem,
        device_id=where,
        device_id_type=pl.DeviceIdType.MESH,
    )


def kernel(
    n_rows, n_cols, table, a_hbm, panel_hbm, u_hbm, k_hbm, sel_out, diag_out,
    av, pv, uv, pr, gather, pick_out, pick_in, acc, r_buf, sel_buf, kv, qsend_buf, qrecv_buf, tot,
    local_sem, p_send, p_recv, a_send, a_recv, g_send, g_recv, q_send, q_recv, t_send, t_recv, f_send,
):
    row = lax.axis_index("prow")
    col = lax.axis_index("pcol")
    width = u_hbm.shape[-1]
    part = panel_hbm.shape[2]
    pairs = n_cols // 2
    row_blocks = a_hbm.shape[1] // width
    col_blocks = a_hbm.shape[2] // width

    def peer(unit):
        return ((col // 2 + unit // 2) % pairs) * 2 + (col + unit) % 2

    copy_p = pltpu.make_async_copy(panel_hbm, pv, local_sem.at[0])
    copy_u = pltpu.make_async_copy(u_hbm.at[:, col], uv, local_sem.at[1])
    copy_a = pltpu.make_async_copy(a_hbm, av, local_sem.at[2])
    copy_k = pltpu.make_async_copy(k_hbm, kv, local_sem.at[3])
    copy_p.start()
    copy_u.start()

    barrier = pltpu.get_barrier_semaphore()
    for unit in range(1, n_cols):
        pl.semaphore_signal(barrier, inc=1, device_id={"pcol": peer(unit)}, device_id_type=pl.DeviceIdType.MESH)

    @pl.when(row > 0)
    def _():
        pl.semaphore_signal(barrier, inc=1, device_id={"prow": row - 1}, device_id_type=pl.DeviceIdType.MESH)

    @pl.when(row < n_rows - 1)
    def _():
        pl.semaphore_signal(barrier, inc=1, device_id={"prow": row + 1}, device_id_type=pl.DeviceIdType.MESH)

    ends = (row == 0).astype(jnp.int32) + (row == n_rows - 1).astype(jnp.int32)
    pl.semaphore_wait(barrier, n_cols + 1 - ends)

    def panel_copy(unit, source):
        return remote(
            pv.at[:, peer(unit)], pr.at[source], p_send.at[unit], p_recv.at[source], {"pcol": peer(unit)}
        )

    def pick_copy(unit, source):
        return remote(
            pick_out.at[unit], pick_in.at[source], a_send.at[unit], a_recv.at[source], {"pcol": peer(unit)}
        )

    def line_copy(unit, chunk, step, side):
        block = gather.at[unit, :, chunk]
        there = row + 1 if side == 0 else row - 1
        return remote(block, block, g_send.at[unit, side, step], g_recv.at[unit, chunk], {"prow": there})

    copy_p.wait()
    copy_a.start()
    for unit in range(1, n_cols):
        panel_copy(unit, col).start()
    copy_u.wait()

    def scale(unit):
        slot = peer(unit)
        if unit == 0:
            left = (pv[0, col], pv[1, col])
        else:
            panel_copy(unit, slot).wait_recv()
            left = (pr[slot, 0], pr[slot, 1])
        real, imag = cdot(left, (uv[0], uv[1]))
        live = (jnp.full((1, width), table[col, slot]) >= 0).astype(F32)
        gather[unit, 0, row] = (real * live).astype(BF16)
        gather[unit, 1, row] = (imag * live).astype(BF16)

        @pl.when(row < n_rows - 1)
        def _():
            line_copy(unit, row, 0, 0).start()

        @pl.when(row > 0)
        def _():
            line_copy(unit, row, 0, 1).start()

    def pick(unit):
        node = peer(unit)
        top = jnp.full((1, width), table[node, row]) - row * row_blocks
        side = jnp.full((1, width), table[node, col]) - col * col_blocks
        for plane in range(2):
            total = None
            for i in range(row_blocks):
                for j in range(col_blocks):
                    keep = ((top == i) & (side == j)).astype(F32).astype(BF16)
                    block = av[plane, i * width : (i + 1) * width, j * width : (j + 1) * width] * keep
                    total = block if total is None else total + block
            pick_out[unit, plane] = total

    scale(0)
    scale(1)
    copy_a.wait()
    copy_k.start()
    order = list(range(2, n_cols)) + [1]
    for unit in order:
        pick(unit)
        pick_copy(unit, col).start()
    pick(0)

    def forward(unit, step):
        below, above = row - step, row + step

        @pl.when(below >= 0)
        def _():
            line_copy(unit, below, step, 0).wait_recv()

            @pl.when(row < n_rows - 1)
            def _():
                line_copy(unit, below, step, 0).start()

        @pl.when(above <= n_rows - 1)
        def _():
            line_copy(unit, above, step, 1).wait_recv()

            @pl.when(row > 0)
            def _():
                line_copy(unit, above, step, 1).start()

    def multiply(unit):
        slot = peer(unit)
        if unit == 0:
            left = (pick_out[0, 0], pick_out[0, 1])
        else:
            pick_copy(unit, slot).wait_recv()
            left = (pick_in[slot, 0], pick_in[slot, 1])
        right = tuple(gather[unit, plane].reshape(width, width) for plane in range(2))
        real, imag = cdot(left, right)
        if unit == 0:
            acc[0] = real
            acc[1] = imag
        else:
            acc[0] += real
            acc[1] += imag

    early, late = (0, 1), range(2, n_cols)
    for unit in early:
        forward(unit, 1)
    for unit in late:
        scale(unit)
    for step in range(2, n_rows + 1):
        for unit in early:
            if step < n_rows:
                forward(unit, step)
        for unit in late:
            forward(unit, step - 1)
            if step == n_rows:
                multiply(unit)
        if step == n_rows - 1:
            for unit in early:
                multiply(unit)
    live = (jnp.full((1, width), table[col, row]) >= 0).astype(F32)
    unit_here = ((row // 2 - col // 2 + pairs) % pairs) * 2 + (row + col) % 2
    z = tuple(gather[unit_here, plane].reshape(width, width) for plane in range(2))
    r = (acc[0] * live, acc[1] * live)
    r_buf[0] = r[0]
    r_buf[1] = r[1]
    halves, pieces = 2, 2
    half_width = width // halves

    def band(piece):
        return pl.ds(piece * (part // pieces), part // pieces)

    def quad_copy(half, piece, step, source):
        there = (row + step) % n_rows
        return remote(
            qsend_buf.at[half, there, :, band(piece)], qrecv_buf.at[half, source, :, band(piece)],
            q_send.at[half, piece, step], q_recv.at[half, piece, source], {"prow": there},
        )

    middle = n_rows // 2

    def total_copy(half, piece, source, target, sem):
        block = tot.at[half, source, :, band(piece)]
        return remote(block, block, sem.at[half, piece, target], t_recv.at[half, piece, source], {"prow": target})

    def direct(target):
        if target in (middle - 1, middle):
            return row != target
        return (row != target) & ((row < middle) if target < middle else (row >= middle))

    def gate(source):
        return row == (middle if source < middle else middle - 1)

    def pass_on(half, piece):
        for source in range(n_rows):
            outer = range(middle + 1, n_rows) if source < middle else range(middle - 1)

            @pl.when(gate(source))
            def _():
                total_copy(half, piece, source, source, t_send).wait_recv()
                for target in outer:
                    total_copy(half, piece, source, target, f_send.at[source]).start()

    low = (r[0].astype(BF16), r[1].astype(BF16))
    for half in range(halves):
        columns = slice(half * half_width, (half + 1) * half_width)
        quad = cdot(z, (low[0][:, columns], low[1][:, columns]), (((0,), (0,)), ((), ())))
        for plane in range(2):
            acc[plane, :, columns] = quad[plane]
            qsend_buf[half, :, plane] = quad[plane].reshape(n_rows, part, half_width).astype(BF16)
        for piece in range(pieces):
            for step in range(1, n_rows):
                quad_copy(half, piece, step, row).start()
    named = jnp.full((1, width), table[col, row]) - row * row_blocks
    for i in range(row_blocks):
        keep = -(named == i).astype(F32)
        for plane in range(2):
            sel_buf[plane, i * width : (i + 1) * width, :] = r_buf[plane] * keep
    copy_s = pltpu.make_async_copy(sel_buf, sel_out, local_sem.at[4])
    copy_s.start()
    copy_k.wait()
    rows_piece = part // pieces
    order_here = []
    for half in range(halves):
        columns = slice(half * half_width, (half + 1) * half_width)
        for piece in range(pieces):
            mine = pl.ds(pl.multiple_of(row * part + piece * rows_piece, rows_piece), rows_piece)
            sums = [acc[0, mine, columns], acc[1, mine, columns]]
            for step in range(1, n_rows):
                source = (row + step) % n_rows
                quad_copy(half, piece, step, source).wait_recv()
                for plane in range(2):
                    sums[plane] = sums[plane] + qrecv_buf[half, source, plane, band(piece)].astype(F32)
            for plane in range(2):
                tot[half, row, plane, band(piece)] = sums[plane].astype(BF16)
            for target in range(n_rows):

                @pl.when(direct(target))
                def _():
                    total_copy(half, piece, row, target, t_send).start()

            order_here.append((half, piece))
            if len(order_here) > 2:
                pass_on(*order_here[-3])
    for entry in order_here[-2:]:
        pass_on(*entry)
    for half in range(halves):
        columns = slice(half * half_width, (half + 1) * half_width)
        for source in range(n_rows):
            for piece in range(pieces):

                @pl.when((row != source) & jnp.logical_not(gate(source)))
                def _():
                    total_copy(half, piece, source, source, t_send).wait_recv()

        for plane in range(2):
            diag_out[plane, 0, :, columns] = (
                kv[plane, 0, :, columns] + tot[half, :, plane].reshape(width, half_width).astype(F32)
            )

    copy_s.wait()
    for unit in range(1, n_cols):
        panel_copy(unit, col).wait_send()
        pick_copy(unit, col).wait_send()
    for unit in range(n_cols):
        for step in range(n_rows):
            below, above = row - step, row + step

            @pl.when((below >= 0) & (row < n_rows - 1))
            def _():
                line_copy(unit, below, step, 0).wait_send()

            @pl.when((above <= n_rows - 1) & (row > 0))
            def _():
                line_copy(unit, above, step, 1).wait_send()

    for step in range(1, n_rows):
        for half in range(halves):
            for piece in range(pieces):
                quad_copy(half, piece, step, row).wait_send()

    for half in range(halves):
        for piece in range(pieces):
            for target in range(n_rows):

                @pl.when(direct(target))
                def _():
                    total_copy(half, piece, row, target, t_send).wait_send()

            for source in range(n_rows):
                outer = range(middle + 1, n_rows) if source < middle else range(middle - 1)

                @pl.when(gate(source))
                def _():
                    for target in outer:
                        total_copy(half, piece, source, target, f_send.at[source]).wait_send()


def compact(ainv_anc, panel, u_inv, k_inv, structure):
    n_rows, n_cols = lax.axis_size("prow"), lax.axis_size("pcol")
    width, part = u_inv.shape[-1], panel.shape[2]
    row_blocks = ainv_anc.shape[1] // width
    hbm = pl.BlockSpec(memory_space=pltpu.HBM)
    vmem = pl.BlockSpec(memory_space=pltpu.VMEM)
    dma = pltpu.SemaphoreType.DMA
    return pl.pallas_call(
        functools.partial(kernel, n_rows, n_cols),
        out_shape=(
            jax.ShapeDtypeStruct((2, row_blocks * width, width), F32),
            jax.ShapeDtypeStruct(k_inv.shape, F32),
        ),
        in_specs=[pl.BlockSpec(memory_space=pltpu.SMEM), hbm, hbm, hbm, hbm],
        out_specs=(hbm, vmem),
        scratch_shapes=[
            pltpu.VMEM(ainv_anc.shape, BF16),
            pltpu.VMEM(panel.shape, BF16),
            pltpu.VMEM((2, width, width), BF16),
            pltpu.VMEM((n_cols, 2, part, width), BF16),
            pltpu.VMEM((n_cols, 2, n_rows, part, width), BF16),
            pltpu.VMEM((n_cols, 2, width, width), BF16),
            pltpu.VMEM((n_cols, 2, width, width), BF16),
            pltpu.VMEM((2, width, width), F32),
            pltpu.VMEM((2, width, width), F32),
            pltpu.VMEM((2, row_blocks * width, width), F32),
            pltpu.VMEM(k_inv.shape, F32),
            pltpu.VMEM((2, n_rows, 2, part, width // 2), BF16),
            pltpu.VMEM((2, n_rows, 2, part, width // 2), BF16),
            pltpu.VMEM((2, n_rows, 2, part, width // 2), BF16),
            dma((5,)),
            dma((n_cols,)),
            dma((n_cols,)),
            dma((n_cols,)),
            dma((n_cols,)),
            dma((n_cols, 2, n_rows)),
            dma((n_cols, n_rows)),
            dma((2, 2, n_rows)),
            dma((2, 2, n_rows)),
            dma((2, 2, n_rows)),
            dma((2, 2, n_rows)),
            dma((n_rows, 2, 2, n_rows)),
        ],
        compiler_params=pltpu.CompilerParams(
            collective_id=0, has_side_effects=True
        ),
    )(structure, ainv_anc, panel, u_inv, k_inv)


def complex_quad(z_part, s_part):
    highest = lax.Precision.HIGHEST

    def single(left, right):
        return jnp.einsum("kra,rkb->kab", left, right, precision=highest)

    real = single(z_part[0], s_part[0]) - single(z_part[1], s_part[1])
    imag = single(z_part[0], s_part[1]) + single(z_part[1], s_part[0])
    return jnp.stack([real, imag])


def local(ainv_anc, panel, u_inv, k_inv, structure):
    block_width = u_inv.shape[-1]
    cols = lax.axis_size("pcol")
    if (
        structure.shape[1] == cols
        and lax.axis_size("prow") == cols
        and ainv_anc.shape[1] == ainv_anc.shape[2]
        and u_inv.shape[1] == cols
        and cols % 2 == 0
    ):
        return compact(ainv_anc, panel, u_inv, k_inv, structure)
    total_k = u_inv.shape[1]
    own_k = k_inv.shape[1]
    n_cols = lax.axis_size("pcol")
    row_here = lax.axis_index("prow")
    col_here = lax.axis_index("pcol")
    row_blocks = ainv_anc.shape[1] // block_width
    group_blocks = ainv_anc.shape[2] // block_width
    group_slots = structure.shape[1] // n_cols
    rows_all = row_blocks * block_width
    col_struct = lax.dynamic_slice_in_dim(structure, col_here * group_slots, group_slots, 1)
    slot_live = col_struct >= 0
    slot_pos = col_struct - col_here * group_blocks
    first_block = row_here * row_blocks
    target = first_block + jnp.arange(row_blocks, dtype=jnp.int32)
    rows_in = lax.all_gather(panel, "prow", axis=2, tiled=True)

    def single(left, right):
        return jnp.einsum("knb,kbc->knc", left, right, preferred_element_type=jnp.float32)

    real = single(rows_in[0], u_inv[0]) - single(rows_in[1], u_inv[1])
    imag = single(rows_in[0], u_inv[1]) + single(rows_in[1], u_inv[0])
    placed = jnp.stack([real, imag]).astype(jnp.bfloat16)
    placed = placed.reshape(2, total_k, group_slots, block_width, block_width)
    placed = jnp.where(slot_live[None, :, :, None, None], placed, jnp.zeros((), jnp.bfloat16))
    block_ids = jnp.arange(group_blocks, dtype=jnp.int32)
    pick_table = (slot_pos[:, :, None] == block_ids[None, None, :]).astype(jnp.bfloat16)
    ainv_blocks = ainv_anc.reshape(2, rows_all, group_blocks, block_width)

    def one_node(items):
        table_k, rows_k = items
        picked = jnp.einsum(
            "sg,cigw->cisw", table_k, ainv_blocks, preferred_element_type=jnp.float32
        )
        picked = picked.astype(jnp.bfloat16).reshape(2, rows_all, group_slots * block_width)
        right = rows_k.reshape(2, group_slots * block_width, block_width)
        real = jnp.dot(picked[0], right[0], preferred_element_type=jnp.float32) - jnp.dot(
            picked[1], right[1], preferred_element_type=jnp.float32
        )
        imag = jnp.dot(picked[0], right[1], preferred_element_type=jnp.float32) + jnp.dot(
            picked[1], right[0], preferred_element_type=jnp.float32
        )
        return jnp.stack([real, imag])

    per_node = lax.map(one_node, (pick_table, jnp.moveaxis(placed, 1, 0)))
    partial_value = jnp.transpose(per_node, (1, 2, 0, 3))
    row_table = (col_struct[:, None, :] == target[None, :, None]).astype(jnp.bfloat16)
    z_rows = jnp.einsum("kts,ckswb->cktwb", row_table, placed, preferred_element_type=jnp.float32)
    z_rows = z_rows.astype(jnp.bfloat16).reshape(2, total_k, rows_all, block_width)
    summed = lax.psum_scatter(
        partial_value.reshape(2, rows_all, total_k * block_width),
        "pcol",
        scatter_dimension=2,
        tiled=True,
    )
    own_struct = lax.dynamic_slice_in_dim(structure, col_here * own_k, own_k, 0)
    member = jnp.any(own_struct[:, :, None] == target[None, None, :], axis=1)
    selected = -summed.reshape(2, row_blocks, block_width, own_k, block_width)
    selected = jnp.where(member.T[None, :, None, :, None], selected, 0.0)
    sel_inv = selected.reshape(2, rows_all, own_k * block_width)
    received = lax.all_to_all(z_rows, "pcol", split_axis=1, concat_axis=1, tiled=True)
    z_own = (
        received.astype(jnp.float32).reshape(2, n_cols, own_k, rows_all, block_width).sum(axis=1)
    )
    quad_term = complex_quad(z_own, selected.reshape(2, rows_all, own_k, block_width))
    total_sum = lax.psum(quad_term, "prow")
    diag_inv = k_inv - total_sum
    return (sel_inv, diag_inv)


def solution(mesh):
    placed = (
        P(None, ("pole", "prow"), "pcol"),
        P(None, "pole", ("pcol", "prow"), None),
        P(None, "pole", None, None),
        P(None, ("pole", "pcol"), None, None),
        P(),
    )
    return jax.shard_map(
        local,
        mesh=mesh,
        in_specs=placed,
        out_specs=(P(None, ("pole", "prow"), "pcol"), P(None, ("pole", "pcol"), None, None)),
        check_vma=False,
    )
```

```python
import functools

import jax
import jax.numpy as jnp
from jax import lax
from jax.experimental import pallas as pl
from jax.experimental.pallas import tpu as pltpu
from jax.sharding import PartitionSpec as P

BF16 = jnp.bfloat16
F32 = jnp.float32


def cdot(left, right, dims=(((1,), (0,)), ((), ()))):
    def single(x, y):
        return lax.dot_general(x, y, dims, preferred_element_type=F32)

    real = single(left[0], right[0]) - single(left[1], right[1])
    imag = single(left[0], right[1]) + single(left[1], right[0])
    return real, imag


def remote(src, dst, send_sem, recv_sem, where):
    return pltpu.make_async_remote_copy(
        src_ref=src,
        dst_ref=dst,
        send_sem=send_sem,
        recv_sem=recv_sem,
        device_id=where,
        device_id_type=pl.DeviceIdType.MESH,
    )


def kernel(
    n_rows, n_cols, table, a_hbm, panel_hbm, u_hbm, k_hbm, sel_out, diag_out,
    av, pv, uv, pr, gather, pick_out, pick_in, acc, r_buf, sel_buf, kv, qsend_buf, qrecv_buf, tot,
    local_sem, p_send, p_recv, a_send, a_recv, g_send, g_recv, q_send, q_recv, t_send, t_recv,
):
    row = lax.axis_index("prow")
    col = lax.axis_index("pcol")
    width = u_hbm.shape[-1]
    part = panel_hbm.shape[2]
    pairs = n_cols // 2
    row_blocks = a_hbm.shape[1] // width
    col_blocks = a_hbm.shape[2] // width

    def peer(unit):
        return ((col // 2 + unit // 2) % pairs) * 2 + (col + unit) % 2

    copy_p = pltpu.make_async_copy(panel_hbm, pv, local_sem.at[0])
    copy_u = pltpu.make_async_copy(u_hbm.at[:, col], uv, local_sem.at[1])
    copy_a = pltpu.make_async_copy(a_hbm, av, local_sem.at[2])
    copy_k = pltpu.make_async_copy(k_hbm, kv, local_sem.at[3])
    copy_p.start()
    copy_u.start()

    barrier = pltpu.get_barrier_semaphore()
    for unit in range(1, n_cols):
        pl.semaphore_signal(barrier, inc=1, device_id={"pcol": peer(unit)}, device_id_type=pl.DeviceIdType.MESH)

    @pl.when(row > 0)
    def _():
        pl.semaphore_signal(barrier, inc=1, device_id={"prow": row - 1}, device_id_type=pl.DeviceIdType.MESH)

    @pl.when(row < n_rows - 1)
    def _():
        pl.semaphore_signal(barrier, inc=1, device_id={"prow": row + 1}, device_id_type=pl.DeviceIdType.MESH)

    ends = (row == 0).astype(jnp.int32) + (row == n_rows - 1).astype(jnp.int32)
    pl.semaphore_wait(barrier, n_cols + 1 - ends)

    def panel_copy(unit, source):
        return remote(
            pv.at[:, peer(unit)], pr.at[source], p_send.at[unit], p_recv.at[source], {"pcol": peer(unit)}
        )

    def pick_copy(unit, source):
        return remote(
            pick_out.at[unit], pick_in.at[source], a_send.at[unit], a_recv.at[source], {"pcol": peer(unit)}
        )

    def line_copy(unit, chunk, step, side):
        block = gather.at[unit, :, chunk]
        there = row + 1 if side == 0 else row - 1
        return remote(block, block, g_send.at[unit, side, step], g_recv.at[unit, chunk], {"prow": there})

    copy_p.wait()
    copy_a.start()
    for unit in range(1, n_cols):
        panel_copy(unit, col).start()
    copy_u.wait()

    def scale(unit):
        slot = peer(unit)
        if unit == 0:
            left = (pv[0, col], pv[1, col])
        else:
            panel_copy(unit, slot).wait_recv()
            left = (pr[slot, 0], pr[slot, 1])
        real, imag = cdot(left, (uv[0], uv[1]))
        live = (jnp.full((1, width), table[col, slot]) >= 0).astype(F32)
        gather[unit, 0, row] = (real * live).astype(BF16)
        gather[unit, 1, row] = (imag * live).astype(BF16)

        @pl.when(row < n_rows - 1)
        def _():
            line_copy(unit, row, 0, 0).start()

        @pl.when(row > 0)
        def _():
            line_copy(unit, row, 0, 1).start()

    def pick(unit):
        node = peer(unit)
        top = jnp.full((1, width), table[node, row]) - row * row_blocks
        side = jnp.full((1, width), table[node, col]) - col * col_blocks
        for plane in range(2):
            total = None
            for i in range(row_blocks):
                for j in range(col_blocks):
                    keep = ((top == i) & (side == j)).astype(F32).astype(BF16)
                    block = av[plane, i * width : (i + 1) * width, j * width : (j + 1) * width] * keep
                    total = block if total is None else total + block
            pick_out[unit, plane] = total

    scale(0)
    scale(1)
    copy_a.wait()
    copy_k.start()
    order = list(range(2, n_cols)) + [1]
    for unit in order:
        pick(unit)
        pick_copy(unit, col).start()
    pick(0)

    def forward(unit, step):
        below, above = row - step, row + step

        @pl.when(below >= 0)
        def _():
            line_copy(unit, below, step, 0).wait_recv()

            @pl.when(row < n_rows - 1)
            def _():
                line_copy(unit, below, step, 0).start()

        @pl.when(above <= n_rows - 1)
        def _():
            line_copy(unit, above, step, 1).wait_recv()

            @pl.when(row > 0)
            def _():
                line_copy(unit, above, step, 1).start()

    def multiply(unit):
        slot = peer(unit)
        if unit == 0:
            left = (pick_out[0, 0], pick_out[0, 1])
        else:
            pick_copy(unit, slot).wait_recv()
            left = (pick_in[slot, 0], pick_in[slot, 1])
        right = tuple(gather[unit, plane].reshape(width, width) for plane in range(2))
        real, imag = cdot(left, right)
        if unit == 0:
            acc[0] = real
            acc[1] = imag
        else:
            acc[0] += real
            acc[1] += imag

    early, late = (0, 1), range(2, n_cols)
    for unit in early:
        forward(unit, 1)
    for unit in late:
        scale(unit)
    for step in range(2, n_rows + 1):
        for unit in early:
            if step < n_rows:
                forward(unit, step)
        for unit in late:
            forward(unit, step - 1)
            if step == n_rows:
                multiply(unit)
        if step == n_rows - 1:
            for unit in early:
                multiply(unit)
    live = (jnp.full((1, width), table[col, row]) >= 0).astype(F32)
    unit_here = ((row // 2 - col // 2 + pairs) % pairs) * 2 + (row + col) % 2
    z = tuple(gather[unit_here, plane].reshape(width, width) for plane in range(2))
    r = (acc[0] * live, acc[1] * live)
    r_buf[0] = r[0]
    r_buf[1] = r[1]
    halves, pieces = 2, 2
    half_width = width // halves

    def diag_copy(half):
        columns = pl.ds(half * half_width, half_width)
        return pltpu.make_async_copy(
            kv.at[:, :, :, columns], diag_out.at[:, :, :, columns], local_sem.at[5 + half]
        )

    def band(piece):
        return pl.ds(piece * (part // pieces), part // pieces)

    def quad_copy(half, piece, step, source):
        there = (row + step) % n_rows
        return remote(
            qsend_buf.at[half, there, :, band(piece)], qrecv_buf.at[half, source, :, band(piece)],
            q_send.at[half, piece, step], q_recv.at[half, piece, source], {"prow": there},
        )

    def total_copy(half, piece, step, source):
        there = (row + step) % n_rows
        block = tot.at[half, source, :, band(piece)]
        return remote(block, block, t_send.at[half, piece, step], t_recv.at[half, piece, source], {"prow": there})

    low = (r[0].astype(BF16), r[1].astype(BF16))
    for half in range(halves):
        columns = slice(half * half_width, (half + 1) * half_width)
        quad = cdot(z, (low[0][:, columns], low[1][:, columns]), (((0,), (0,)), ((), ())))
        for plane in range(2):
            acc[plane, :, columns] = quad[plane]
            qsend_buf[half, :, plane] = quad[plane].reshape(n_rows, part, half_width).astype(BF16)
        for piece in range(pieces):
            for step in range(1, n_rows):
                quad_copy(half, piece, step, row).start()
    named = jnp.full((1, width), table[col, row]) - row * row_blocks
    for i in range(row_blocks):
        keep = -(named == i).astype(F32)
        for plane in range(2):
            sel_buf[plane, i * width : (i + 1) * width, :] = r_buf[plane] * keep
    copy_s = pltpu.make_async_copy(sel_buf, sel_out, local_sem.at[4])
    copy_s.start()
    copy_k.wait()
    rows_piece = part // pieces
    for half in range(halves):
        columns = slice(half * half_width, (half + 1) * half_width)
        for piece in range(pieces):
            mine = pl.ds(pl.multiple_of(row * part + piece * rows_piece, rows_piece), rows_piece)
            sums = [acc[0, mine, columns], acc[1, mine, columns]]
            for step in range(1, n_rows):
                source = (row + step) % n_rows
                quad_copy(half, piece, step, source).wait_recv()
                for plane in range(2):
                    sums[plane] = sums[plane] + qrecv_buf[half, source, plane, band(piece)].astype(F32)
            for plane in range(2):
                tot[half, row, plane, band(piece)] = sums[plane].astype(BF16)
            for step in range(1, n_rows):
                total_copy(half, piece, step, row).start()
    for half in range(halves):
        columns = slice(half * half_width, (half + 1) * half_width)
        for step in range(1, n_rows):
            for piece in range(pieces):
                total_copy(half, piece, step, (row + step) % n_rows).wait_recv()
        for plane in range(2):
            kv[plane, 0, :, columns] = (
                kv[plane, 0, :, columns] + tot[half, :, plane].reshape(width, half_width).astype(F32)
            )

        diag_copy(half).start()
    copy_s.wait()
    for half in range(halves):
        diag_copy(half).wait()
    for unit in range(1, n_cols):
        panel_copy(unit, col).wait_send()
        pick_copy(unit, col).wait_send()
    for unit in range(n_cols):
        for step in range(n_rows):
            below, above = row - step, row + step

            @pl.when((below >= 0) & (row < n_rows - 1))
            def _():
                line_copy(unit, below, step, 0).wait_send()

            @pl.when((above <= n_rows - 1) & (row > 0))
            def _():
                line_copy(unit, above, step, 1).wait_send()

    for step in range(1, n_rows):
        for half in range(halves):
            for piece in range(pieces):
                quad_copy(half, piece, step, row).wait_send()
                total_copy(half, piece, step, row).wait_send()


def place(cuts, sel_hbm, diag_hbm, sel_out, diag_out, sel_buf, diag_buf, in_sem, out_sem):
    rows = sel_hbm.shape[1] // cuts
    ins, outs = [], []
    for plane in range(2):
        for cut in range(cuts):
            at = (plane, pl.ds(cut * rows, rows))
            index = plane * (cuts + 1) + cut
            ins.append(pltpu.make_async_copy(sel_hbm.at[at], sel_buf.at[at], in_sem.at[index]))
            outs.append(pltpu.make_async_copy(sel_buf.at[at], sel_out.at[at], out_sem.at[index]))
        index = plane * (cuts + 1) + cuts
        ins.append(pltpu.make_async_copy(diag_hbm.at[plane], diag_buf.at[plane], in_sem.at[index]))
        outs.append(pltpu.make_async_copy(diag_buf.at[plane], diag_out.at[plane], out_sem.at[index]))
    for copy in ins:
        copy.start()
    for load, store in zip(ins, outs):
        load.wait()
        store.start()
    for copy in outs:
        copy.wait()


def compact(ainv_anc, panel, u_inv, k_inv, structure):
    n_rows, n_cols = lax.axis_size("prow"), lax.axis_size("pcol")
    width, part = u_inv.shape[-1], panel.shape[2]
    row_blocks = ainv_anc.shape[1] // width
    hbm = pl.BlockSpec(memory_space=pltpu.HBM)
    vmem = pl.BlockSpec(memory_space=pltpu.VMEM)
    dma = pltpu.SemaphoreType.DMA
    shapes = (
        jax.ShapeDtypeStruct((2, row_blocks * width, width), F32),
        jax.ShapeDtypeStruct(k_inv.shape, F32),
    )
    results = pl.pallas_call(
        functools.partial(kernel, n_rows, n_cols),
        out_shape=shapes,
        in_specs=[pl.BlockSpec(memory_space=pltpu.SMEM), hbm, hbm, hbm, hbm],
        out_specs=(hbm, hbm),
        scratch_shapes=[
            pltpu.VMEM(ainv_anc.shape, BF16),
            pltpu.VMEM(panel.shape, BF16),
            pltpu.VMEM((2, width, width), BF16),
            pltpu.VMEM((n_cols, 2, part, width), BF16),
            pltpu.VMEM((n_cols, 2, n_rows, part, width), BF16),
            pltpu.VMEM((n_cols, 2, width, width), BF16),
            pltpu.VMEM((n_cols, 2, width, width), BF16),
            pltpu.VMEM((2, width, width), F32),
            pltpu.VMEM((2, width, width), F32),
            pltpu.VMEM((2, row_blocks * width, width), F32),
            pltpu.VMEM(k_inv.shape, F32),
            pltpu.VMEM((2, n_rows, 2, part, width // 2), BF16),
            pltpu.VMEM((2, n_rows, 2, part, width // 2), BF16),
            pltpu.VMEM((2, n_rows, 2, part, width // 2), BF16),
            dma((7,)),
            dma((n_cols,)),
            dma((n_cols,)),
            dma((n_cols,)),
            dma((n_cols,)),
            dma((n_cols, 2, n_rows)),
            dma((n_cols, n_rows)),
            dma((2, 2, n_rows)),
            dma((2, 2, n_rows)),
            dma((2, 2, n_rows)),
            dma((2, 2, n_rows)),
        ],
        compiler_params=pltpu.CompilerParams(
            collective_id=0, has_side_effects=True
        ),
    )(structure, ainv_anc, panel, u_inv, k_inv)
    cuts = 2
    return pl.pallas_call(
        functools.partial(place, cuts),
        out_shape=shapes,
        in_specs=[hbm, hbm],
        out_specs=(hbm, hbm),
        scratch_shapes=[
            pltpu.VMEM(shapes[0].shape, F32),
            pltpu.VMEM(shapes[1].shape, F32),
            dma((2 * (cuts + 1),)),
            dma((2 * (cuts + 1),)),
        ],
    )(*results)


def complex_quad(z_part, s_part):
    highest = lax.Precision.HIGHEST

    def single(left, right):
        return jnp.einsum("kra,rkb->kab", left, right, precision=highest)

    real = single(z_part[0], s_part[0]) - single(z_part[1], s_part[1])
    imag = single(z_part[0], s_part[1]) + single(z_part[1], s_part[0])
    return jnp.stack([real, imag])


def local(ainv_anc, panel, u_inv, k_inv, structure):
    block_width = u_inv.shape[-1]
    cols = lax.axis_size("pcol")
    if (
        structure.shape[1] == cols
        and lax.axis_size("prow") == cols
        and ainv_anc.shape[1] == ainv_anc.shape[2]
        and u_inv.shape[1] == cols
        and cols % 2 == 0
    ):
        return compact(ainv_anc, panel, u_inv, k_inv, structure)
    total_k = u_inv.shape[1]
    own_k = k_inv.shape[1]
    n_cols = lax.axis_size("pcol")
    row_here = lax.axis_index("prow")
    col_here = lax.axis_index("pcol")
    row_blocks = ainv_anc.shape[1] // block_width
    group_blocks = ainv_anc.shape[2] // block_width
    group_slots = structure.shape[1] // n_cols
    rows_all = row_blocks * block_width
    col_struct = lax.dynamic_slice_in_dim(structure, col_here * group_slots, group_slots, 1)
    slot_live = col_struct >= 0
    slot_pos = col_struct - col_here * group_blocks
    first_block = row_here * row_blocks
    target = first_block + jnp.arange(row_blocks, dtype=jnp.int32)
    rows_in = lax.all_gather(panel, "prow", axis=2, tiled=True)

    def single(left, right):
        return jnp.einsum("knb,kbc->knc", left, right, preferred_element_type=jnp.float32)

    real = single(rows_in[0], u_inv[0]) - single(rows_in[1], u_inv[1])
    imag = single(rows_in[0], u_inv[1]) + single(rows_in[1], u_inv[0])
    placed = jnp.stack([real, imag]).astype(jnp.bfloat16)
    placed = placed.reshape(2, total_k, group_slots, block_width, block_width)
    placed = jnp.where(slot_live[None, :, :, None, None], placed, jnp.zeros((), jnp.bfloat16))
    block_ids = jnp.arange(group_blocks, dtype=jnp.int32)
    pick_table = (slot_pos[:, :, None] == block_ids[None, None, :]).astype(jnp.bfloat16)
    ainv_blocks = ainv_anc.reshape(2, rows_all, group_blocks, block_width)

    def one_node(items):
        table_k, rows_k = items
        picked = jnp.einsum(
            "sg,cigw->cisw", table_k, ainv_blocks, preferred_element_type=jnp.float32
        )
        picked = picked.astype(jnp.bfloat16).reshape(2, rows_all, group_slots * block_width)
        right = rows_k.reshape(2, group_slots * block_width, block_width)
        real = jnp.dot(picked[0], right[0], preferred_element_type=jnp.float32) - jnp.dot(
            picked[1], right[1], preferred_element_type=jnp.float32
        )
        imag = jnp.dot(picked[0], right[1], preferred_element_type=jnp.float32) + jnp.dot(
            picked[1], right[0], preferred_element_type=jnp.float32
        )
        return jnp.stack([real, imag])

    per_node = lax.map(one_node, (pick_table, jnp.moveaxis(placed, 1, 0)))
    partial_value = jnp.transpose(per_node, (1, 2, 0, 3))
    row_table = (col_struct[:, None, :] == target[None, :, None]).astype(jnp.bfloat16)
    z_rows = jnp.einsum("kts,ckswb->cktwb", row_table, placed, preferred_element_type=jnp.float32)
    z_rows = z_rows.astype(jnp.bfloat16).reshape(2, total_k, rows_all, block_width)
    summed = lax.psum_scatter(
        partial_value.reshape(2, rows_all, total_k * block_width),
        "pcol",
        scatter_dimension=2,
        tiled=True,
    )
    own_struct = lax.dynamic_slice_in_dim(structure, col_here * own_k, own_k, 0)
    member = jnp.any(own_struct[:, :, None] == target[None, None, :], axis=1)
    selected = -summed.reshape(2, row_blocks, block_width, own_k, block_width)
    selected = jnp.where(member.T[None, :, None, :, None], selected, 0.0)
    sel_inv = selected.reshape(2, rows_all, own_k * block_width)
    received = lax.all_to_all(z_rows, "pcol", split_axis=1, concat_axis=1, tiled=True)
    z_own = (
        received.astype(jnp.float32).reshape(2, n_cols, own_k, rows_all, block_width).sum(axis=1)
    )
    quad_term = complex_quad(z_own, selected.reshape(2, rows_all, own_k, block_width))
    total_sum = lax.psum(quad_term, "prow")
    diag_inv = k_inv - total_sum
    return (sel_inv, diag_inv)


def solution(mesh):
    placed = (
        P(None, ("pole", "prow"), "pcol"),
        P(None, "pole", ("pcol", "prow"), None),
        P(None, "pole", None, None),
        P(None, ("pole", "pcol"), None, None),
        P(),
    )
    return jax.shard_map(
        local,
        mesh=mesh,
        in_specs=placed,
        out_specs=(P(None, ("pole", "prow"), "pcol"), P(None, ("pole", "pcol"), None, None)),
        check_vma=False,
    )
```
